32 devices in a mesh: wide: 8 (over z, y), narrow: 4 (over x, core).
Axes of the slice: x: 2, y: 2, z: 4, core: 2. Of those that a mesh axis runs over, the one named last changes fastest.
Arguments:
- values: float32 [512, 16384], P(('wide', 'narrow')), may hold values from -200 to 200, as said below
- cloud_words: int32 [512, 512], P(('wide', 'narrow')), may hold values from -2147483648 to 2147483647, as said below
- history_len: int32 [1], replicated, may hold values from 96 to 256
- monitor_start: int32 [1], replicated, may hold values from 256 to 384
- boundary_table: int32 [512], replicated, may hold values from 500 to 2000
Outputs:
- ratio: float32 [512, 16384], P(('wide', 'narrow'))
- peak_so_far: float32 [512, 16384], P(('wide', 'narrow'))
The draws below stay inside these ranges and needn't reach their ends.
Inputs may be any that keep to these rules, and one draw needn't show every extreme that they name: `values`: values of an index series, mixed noise and a seasonal cycle of varying scale. `cloud_words`: bit b of word j in the row of date t is 1 when pixel 32 j + b is clear at date t; the first 16 dates are clear for every pixel.
All inputs are finite; a program needn't handle non-finite values.
Results may differ from the reference program's by a relative error of at most 0.0003.
Values sent between devices are 32-bit elements; how exact they have to be, the bound alone decides.
No kernel may reach another device: no remote copies, remote signals or barrier semaphores. Data moves between devices by JAX's collectives and lax.ppermute only.
A program may use at most 64 MiB of HBM per device.

```python
import math
import jax
import jax.numpy as jnp
from jax import lax

DATES = 512
PIX_DEV = 512
PERIOD = 46
HARMONICS = 3
COLS = 8
WINDOW = 64
PIXELS = 16384


def draw_values(key, part):
    keys = jax.random.split(key, 4)
    day_float = jnp.arange(DATES, dtype=jnp.int32).astype(jnp.float32)[:, None]
    amplitude = jax.random.uniform(keys[2], (PIXELS,), jnp.float32, 0.0, 2.0)
    offset = jax.random.uniform(keys[3], (PIXELS,), jnp.float32, -math.pi, math.pi)
    seasonal = amplitude[None, :] * jnp.cos(2.0 * math.pi / PERIOD * day_float + offset[None, :])
    noise = jnp.clip(jax.random.normal(keys[0], (DATES, PIXELS), jnp.float32), -6.0, 6.0)
    scales = jnp.exp(jax.random.uniform(keys[1], (PIXELS,), jnp.float32, 0.0, math.log(10.0)))
    return scales[None, :] * (noise + seasonal)


def draw_cloud_words(key, part):
    keys = jax.random.split(jax.random.fold_in(key, 17), 2)
    lowest = jnp.iinfo(jnp.int32).min
    highest = jnp.iinfo(jnp.int32).max
    first = jax.random.randint(keys[0], (DATES, PIXELS // 32), lowest, highest, dtype=jnp.int32)
    second = jax.random.randint(keys[1], (DATES, PIXELS // 32), lowest, highest, dtype=jnp.int32)
    words = jnp.bitwise_or(first, second)
    early = (jnp.arange(DATES, dtype=jnp.int32) < 16)[:, None]
    return jnp.where(early, jnp.int32(-1), words)


def with_ends(array, stream_key, smallest, top_value):
    longest = array.shape.index(max(array.shape))
    spots = []
    for shift in (0, 1):
        where = [jax.random.randint(jax.random.fold_in(stream_key, axis), (), 0, length) for axis, length in enumerate(array.shape)]
        where[longest] = (where[longest] + shift) % array.shape[longest]
        spots.append(tuple(where))
    return array.at[spots[0]].set(smallest).at[spots[1]].set(top_value)


def setup_inputs(seed: int = 0) -> dict:
    seeds = jax.random.split(jax.random.key(seed), 6)
    return {
        "values": draw_values(jax.random.fold_in(seeds[5], 71), 0),
        "cloud_words": draw_cloud_words(jax.random.fold_in(seeds[5], 71), 0),
        "history_len": jax.random.randint(seeds[2], (1,), DATES * 3 // 16, DATES // 2 + 1).astype(jnp.int32),
        "monitor_start": jax.random.randint(seeds[3], (1,), DATES // 2, DATES * 3 // 4 + 1).astype(jnp.int32),
        "boundary_table": with_ends(jax.random.randint(seeds[4], (DATES,), 500, 2001), jax.random.fold_in(seeds[4], 1), 500, 2000).astype(jnp.int32),
    }


HIGH = lax.Precision.HIGHEST

def unpack_clear(words):
    shifts = jnp.arange(32, dtype=jnp.int32)
    flags = jnp.bitwise_and(jnp.right_shift(words[:, :, None], shifts[None, None, :]), jnp.int32(1))
    return flags.reshape(words.shape[0], words.shape[1] * 32).astype(jnp.float32)

def harmonic_design(dates):
    day_float = jnp.arange(dates, dtype=jnp.int32).astype(jnp.float32)
    columns = [jnp.ones((dates,), jnp.float32), day_float / dates]
    for harmonic in range(1, HARMONICS + 1):
        phases = 2.0 * math.pi * harmonic / PERIOD * day_float
        columns.append(jnp.cos(phases))
        columns.append(jnp.sin(phases))
    return jnp.stack(columns, axis=1)

def solve_batched(normal_mat, target):
    size_cols = normal_mat.shape[0]
    factor = [[None] * size_cols for row_idx in range(size_cols)]
    for row_idx in range(size_cols):
        for col_idx in range(row_idx + 1):
            summed = normal_mat[row_idx, col_idx]
            for mid_idx in range(col_idx):
                summed = summed - factor[row_idx][mid_idx] * factor[col_idx][mid_idx]
            if row_idx == col_idx:
                factor[row_idx][col_idx] = jnp.sqrt(summed)
            else:
                factor[row_idx][col_idx] = summed / factor[col_idx][col_idx]
    forward = []
    for row_idx in range(size_cols):
        summed = target[row_idx]
        for mid_idx in range(row_idx):
            summed = summed - factor[row_idx][mid_idx] * forward[mid_idx]
        forward.append(summed / factor[row_idx][row_idx])
    solution = [None] * size_cols
    for row_idx in reversed(range(size_cols)):
        summed = forward[row_idx]
        for mid_idx in range(row_idx + 1, size_cols):
            summed = summed - factor[mid_idx][row_idx] * solution[mid_idx]
        solution[row_idx] = summed / factor[row_idx][row_idx]
    return jnp.stack(solution, axis=0)

def fit_statistic(values, clear, history_len, monitor_start, boundary_table):
    dates = values.shape[0]
    day = jnp.arange(dates, dtype=jnp.int32)
    design = harmonic_design(dates)
    in_history = (day < history_len[0]).astype(jnp.float32)[:, None]
    weight = clear * in_history
    outer = (design[:, :, None] * design[:, None, :]).reshape(dates, COLS * COLS)
    normal_mat = jnp.dot(outer.T, weight, precision=HIGH, preferred_element_type=jnp.float32).reshape(COLS, COLS, -1)
    target = jnp.dot(design.T, weight * values, precision=HIGH, preferred_element_type=jnp.float32)
    coeffs = solve_batched(normal_mat, target)
    fitted = jnp.dot(design, coeffs, precision=HIGH, preferred_element_type=jnp.float32)
    resid = clear * (values - fitted)
    count = lax.optimization_barrier(jnp.sum(weight, axis=0))
    squares = lax.optimization_barrier(jnp.sum(weight * resid * resid, axis=0))
    sigma = jnp.sqrt(squares / (count - COLS) + 1e-06)
    lagged = day[:, None] - day[None, :]
    banded = ((lagged >= 0) & (lagged < WINDOW)).astype(jnp.float32)
    moving = jnp.dot(banded, resid, precision=HIGH, preferred_element_type=jnp.float32)
    scaled = moving / (sigma * jnp.sqrt(count))[None, :]
    bounds = boundary_table.astype(jnp.float32) * 0.001
    watching = (day >= monitor_start[0])[:, None]
    return jnp.where(watching, scaled / bounds[:, None], jnp.float32(0.0))

def reassemble(blocked):
    return blocked.transpose(1, 0, 2).reshape(DATES, -1)

def reference(values, cloud_words, history_len, monitor_start, boundary_table):
    block_count = values.shape[1] // PIX_DEV
    value_blocks = values.reshape(DATES, block_count, PIX_DEV).transpose(1, 0, 2)
    word_blocks = cloud_words.reshape(DATES, block_count, PIX_DEV // 32).transpose(1, 0, 2)

    def one_block(block_pair):
        ratio = fit_statistic(block_pair[0], unpack_clear(block_pair[1]), history_len, monitor_start, boundary_table)
        return (ratio, lax.cummax(jnp.abs(ratio), axis=0))
    ratios, peaks = lax.map(one_block, (value_blocks, word_blocks))
    return (reassemble(ratios), reassemble(peaks))
```

```python
import functools
import math

import jax
import jax.numpy as jnp
import numpy as np
from jax import lax
from jax.experimental import pallas as pl
from jax.experimental.pallas import tpu as pltpu
from jax.sharding import PartitionSpec as P

PERIOD = 46
HARMONICS = 3
COLS = 8
WINDOW = 64
WORD = 32
AXES = ("wide", "narrow")
HIGH = lax.Precision.HIGHEST


def design_table(dates):
    day = np.arange(dates).astype(np.float32)
    columns = [np.ones((dates,), np.float32), day / np.float32(dates)]
    for harmonic in range(1, HARMONICS + 1):
        phases = (np.float32(2.0 * math.pi * harmonic / PERIOD) * day).astype(np.float64)
        columns.append(np.cos(phases).astype(np.float32))
        columns.append(np.sin(phases).astype(np.float32))
    return np.stack(columns, axis=1)


def outer_table(design):
    rows = [design[:, i] * design[:, j] for i in range(COLS) for j in range(i + 1)]
    while len(rows) % 8:
        rows.append(np.zeros_like(rows[0]))
    return np.stack(rows, axis=0)


def spread_table(pixels):
    words = pixels // WORD
    pixel = np.arange(pixels)
    table = np.zeros((4, words, pixels), np.float32)
    table[(pixel % WORD) // 8, pixel // WORD, pixel] = 1.0
    return table.reshape(4 * words, pixels)


def unpack_clear(words, spread):
    planes = [jnp.bitwise_and(jnp.right_shift(words, 8 * k), 255).astype(jnp.float32) for k in range(4)]
    byte_of = jnp.dot(jnp.concatenate(planes, axis=1).astype(jnp.bfloat16), spread, preferred_element_type=jnp.float32)
    bit = jnp.bitwise_and(lax.broadcasted_iota(jnp.int32, byte_of.shape, 1), 7)
    return jnp.bitwise_and(jnp.right_shift(byte_of.astype(jnp.int32), bit), 1).astype(jnp.float32)


def solve_rows(normal, target):
    factor = {}
    inverse = []
    for col in range(COLS):
        for row in range(col, COLS):
            summed = normal(row, col)
            for mid in range(col):
                summed = summed - factor[row, mid] * factor[col, mid]
            if row == col:
                inverse.append(1.0 / jnp.sqrt(summed))
            else:
                factor[row, col] = summed * inverse[col]
    forward = []
    for row in range(COLS):
        summed = target(row)
        for mid in range(row):
            summed = summed - factor[row, mid] * forward[mid]
        forward.append(summed * inverse[row])
    solved = [None] * COLS
    for row in reversed(range(COLS)):
        summed = forward[row]
        for mid in range(row + 1, COLS):
            summed = summed - factor[mid, row] * solved[mid]
        solved[row] = summed * inverse[row]
    return solved


def fit_kernel(history_ref, values_ref, words_ref, spread_ref, outer_ref, turned_ref, design_ref, stats_ref):
    clear = unpack_clear(words_ref[...], spread_ref[...])
    day = lax.broadcasted_iota(jnp.int32, clear.shape, 0)
    weight = jnp.where(day < history_ref[0], clear, 0.0)
    values = values_ref[...]
    normal = jnp.dot(outer_ref[...], weight, precision=HIGH, preferred_element_type=jnp.float32)
    target = jnp.dot(turned_ref[...], weight * values, precision=HIGH, preferred_element_type=jnp.float32)
    solved = solve_rows(
        lambda i, j: normal[i * (i + 1) // 2 + j][None, :],
        lambda i: target[i][None, :],
    )
    for i in range(COLS):
        stats_ref[i : i + 1, :] = solved[i]
    coeffs = stats_ref[0:COLS, :]
    fitted = jnp.dot(design_ref[...], coeffs, precision=HIGH, preferred_element_type=jnp.float32)
    resid = weight * (values - fitted)
    squares = jnp.sum(resid * resid, axis=0, keepdims=True)
    count = normal[0:1, :]
    sigma = jnp.sqrt(squares / (count - COLS) + 1e-06)
    stats_ref[COLS : COLS + 1, :] = 1.0 / (sigma * jnp.sqrt(count))
    stats_ref[COLS + 1 :, :] = jnp.zeros_like(stats_ref[COLS + 1 :, :])


def ratio_kernel(values_ref, words_ref, early_ref, early_words_ref, stats_ref, spread_ref, design_ref, late_ref, ratio_ref, carry_ref):
    spread = spread_ref[...]
    fitted = jnp.dot(design_ref[...], stats_ref[0:COLS, :], precision=HIGH, preferred_element_type=jnp.float32)
    before = unpack_clear(early_words_ref[...], spread) * (early_ref[...] - fitted[:WINDOW])
    after = unpack_clear(words_ref[...], spread) * (values_ref[...] - fitted[WINDOW:])
    moving = jnp.concatenate([before, after], axis=0)
    span = 1
    while span < WINDOW:
        moving = moving + pltpu.roll(moving, span, 0)
        span *= 2
    ratio = moving[WINDOW:] * stats_ref[COLS : COLS + 1, :] * late_ref[:, 0:1]
    ratio_ref[...] = ratio
    blocks = carry_ref.shape[0]
    per_block = ratio.shape[0] // blocks
    running = jnp.zeros((1, ratio.shape[1]), jnp.float32)
    for block in range(blocks):
        carry_ref[block : block + 1, :] = running
        top = jnp.max(jnp.abs(ratio[block * per_block : (block + 1) * per_block]), axis=0, keepdims=True)
        running = jnp.maximum(running, top)


def finish_kernel(upper_ref, ratio_ref, carry_ref, out_ref, peak_ref):
    blocks, rows, width = ratio_ref.shape
    upper = upper_ref[0] > 0
    for block in range(blocks):
        at = slice(block * width, (block + 1) * width)
        ratio = jnp.where(upper, ratio_ref[block], 0.0)
        peak = jnp.maximum(jnp.abs(ratio), jnp.where(upper, carry_ref[block : block + 1, :], 0.0))
        row = lax.broadcasted_iota(jnp.int32, peak.shape, 0)
        span = 1
        while span < rows:
            peak = jnp.maximum(peak, jnp.where(row >= span, pltpu.roll(peak, span, 0), 0.0))
            span *= 2
        out_ref[:, at] = ratio
        peak_ref[:, at] = peak


SMEM = pl.BlockSpec(memory_space=pltpu.SMEM)
VMEM = pl.BlockSpec(memory_space=pltpu.VMEM)


def f32(*shape):
    return jax.ShapeDtypeStruct(shape, jnp.float32)


def per_device(values, cloud_words, history_len, monitor_start, boundary_table, devices):
    rows, pixels = values.shape
    dates = boundary_table.shape[0]
    half = devices // 2
    late = dates // 2
    width = pixels // half
    words = width // WORD
    groups = [list(range(half)), list(range(half, devices))]
    upward = [(i, i + half) for i in range(half)]
    design = design_table(dates)
    spread = jnp.asarray(spread_table(width), jnp.bfloat16)

    def exchange(blocks):
        return lax.all_to_all(blocks, AXES, 0, 0, axis_index_groups=groups, tiled=True)

    sent_words = cloud_words.reshape(rows, half, words).transpose(1, 0, 2).reshape(half, rows * words)
    own_words = exchange(sent_words).reshape(late, words)
    own = exchange(values.reshape(rows, half, width).transpose(1, 0, 2)).reshape(late, width)
    early = lax.ppermute(own[late - WINDOW :], AXES, upward)
    early_words = lax.ppermute(own_words[late - WINDOW :], AXES, upward)
    stats = pl.pallas_call(
        fit_kernel,
        out_shape=f32(2 * COLS, width),
        in_specs=[SMEM] + [VMEM] * 6,
        out_specs=VMEM,
        name="fit",
    )(history_len, own, own_words, spread, outer_table(design[:late]), design[:late].T, design[:late])
    stats = lax.ppermute(stats, AXES, upward)
    day = jnp.arange(late, dtype=jnp.int32) + late
    factor = jnp.where(day >= monitor_start[0], 1.0 / (boundary_table[late:].astype(jnp.float32) * 0.001), 0.0)
    factor = jnp.broadcast_to(factor[:, None], (late, 128))
    ratio, carry = pl.pallas_call(
        ratio_kernel,
        out_shape=(f32(late, width), f32(half, width)),
        in_specs=[VMEM] * 8,
        out_specs=(VMEM, VMEM),
        name="ratio",
    )(own, own_words, early, early_words, stats, spread, design[late - WINDOW :], factor)
    ratio = exchange(ratio.reshape(half, rows, width))
    carry = exchange(carry)
    upper = (lax.axis_index(AXES) >= half).astype(jnp.int32).reshape(1)
    return pl.pallas_call(
        finish_kernel,
        out_shape=(f32(rows, pixels), f32(rows, pixels)),
        in_specs=[SMEM, VMEM, VMEM],
        out_specs=(VMEM, VMEM),
        name="finish",
    )(upper, ratio, carry)


def solution(mesh):
    placed = (P(AXES, None), P(AXES, None), P(), P(), P())
    return jax.shard_map(
        functools.partial(per_device, devices=mesh.size),
        mesh=mesh,
        in_specs=placed,
        out_specs=(P(AXES, None), P(AXES, None)),
        check_vma=False,
    )
```

```python
import functools
import math

import jax
import jax.numpy as jnp
import ml_dtypes
import numpy as np
from jax import lax
from jax.experimental import pallas as pl
from jax.experimental.pallas import tpu as pltpu
from jax.sharding import PartitionSpec as P

PERIOD = 46
HARMONICS = 3
COLS = 8
WINDOW = 64
WORD = 32
LANES = 128
SUB = 8
STEPS = 4
AXES = ("wide", "narrow")


def design_table(dates):
    day = np.arange(dates).astype(np.float32)
    columns = [np.ones((dates,), np.float32), day / np.float32(dates)]
    for harmonic in range(1, HARMONICS + 1):
        phases = (np.float32(2.0 * math.pi * harmonic / PERIOD) * day).astype(np.float64)
        columns.append(np.cos(phases).astype(np.float32))
        columns.append(np.sin(phases).astype(np.float32))
    return np.stack(columns, axis=1)


def outer_table(design):
    rows = [design[:, i] * design[:, j] for i in range(COLS) for j in range(i + 1)]
    while len(rows) % SUB:
        rows.append(np.zeros_like(rows[0]))
    return np.stack(rows, axis=0)


def split_table(table):
    parts = []
    rest = table
    for _ in range(3):
        part = rest.astype(ml_dtypes.bfloat16)
        parts.append(part)
        rest = rest - part.astype(np.float32)
    return parts


def split_rows(array):
    high = array.astype(jnp.bfloat16).astype(jnp.float32)
    rest = array - high
    mid = rest.astype(jnp.bfloat16).astype(jnp.float32)
    return high, mid, rest - mid


def spread_table(pixels, slots):
    pixel = np.arange(pixels)
    byte = (pixel % WORD) // 8
    table = np.zeros((slots, 2 * LANES, pixels), np.float32)
    for slot in range(slots):
        table[slot, (byte % 2) * LANES + 64 * slot + 32 * (byte // 2) + pixel // WORD, pixel] = 1.0
    return table.astype(ml_dtypes.bfloat16)


def flat_rows(blocks):
    count, rows, lanes = blocks.shape
    if rows % SUB == 0:
        return blocks.reshape(count * rows, lanes)
    return jnp.concatenate([blocks[i] for i in range(count)], axis=0)


def read_values(message, rows):
    tiles = (message.shape[1] - SUB) // rows
    return jnp.concatenate([flat_rows(message[:, c * rows : (c + 1) * rows]) for c in range(tiles)], axis=1)


def read_clear(message, rows, spread_ref):
    blocks = message.shape[0]
    halves = message[:, -SUB:].reshape(blocks * SUB, LANES).astype(jnp.int32)
    planes = [jnp.bitwise_and(halves, 255), jnp.right_shift(halves, 8)]
    planes = jnp.concatenate([plane.astype(jnp.float32) for plane in planes], axis=1).astype(jnp.bfloat16)
    found = []
    for slot in range(spread_ref.shape[0]):
        byte = jnp.dot(planes, spread_ref[slot], preferred_element_type=jnp.float32).astype(jnp.int32)
        bit = jnp.bitwise_and(lax.broadcasted_iota(jnp.int32, byte.shape, 1), 7)
        flags = jnp.bitwise_and(jnp.right_shift(byte, bit), 1).astype(jnp.float32)
        found.append(flags.reshape(blocks, SUB, -1)[:, : min(rows, SUB)])
    return flat_rows(jnp.concatenate(found, axis=1))


def fit_dot(design_ref, coeffs):
    high, mid, low = split_rows(coeffs)
    stacked = jnp.concatenate([high, high, high, mid, mid, low], axis=0).astype(jnp.bfloat16)
    return jnp.dot(design_ref[...], stacked, preferred_element_type=jnp.float32)


def six_wide(design):
    high, mid, low = split_table(design)
    return np.concatenate([high, mid, low, high, mid, high], axis=1)


def solve_rows(normal, target):
    factor = {}
    inverse = []
    for col in range(COLS):
        for row in range(col, COLS):
            summed = normal(row, col)
            for mid in range(col):
                summed = summed - factor[row, mid] * factor[col, mid]
            if row == col:
                inverse.append(1.0 / jnp.sqrt(summed))
            else:
                factor[row, col] = summed * inverse[col]
    forward = []
    for row in range(COLS):
        summed = target(row)
        for mid in range(row):
            summed = summed - factor[row, mid] * forward[mid]
        forward.append(summed * inverse[row])
    solved = [None] * COLS
    for row in reversed(range(COLS)):
        summed = forward[row]
        for mid in range(row + 1, COLS):
            summed = summed - factor[mid, row] * solved[mid]
        solved[row] = summed * inverse[row]
    return solved


def pack_kernel(values_ref, words_ref, message_ref):
    rows = values_ref.shape[0]
    blocks, length, _ = message_ref.shape
    tiles = (length - SUB) // rows
    for block in range(blocks):
        for c in range(tiles):
            start = (block * tiles + c) * LANES
            message_ref[block, c * rows : (c + 1) * rows, :] = values_ref[:, start : start + LANES]
        per_tile = LANES // WORD
        words = words_ref[:, block // per_tile * LANES : (block // per_tile + 1) * LANES]
        if rows % SUB:
            words = jnp.concatenate([words, jnp.zeros((SUB - rows % SUB, LANES), jnp.int32)], axis=0)
        quarter = lax.broadcasted_iota(jnp.int32, (SUB, LANES), 1) // WORD
        riding = jnp.zeros((SUB, LANES), jnp.int32)
        for slot in range(words.shape[0] // SUB):
            part = words[slot * SUB : (slot + 1) * SUB]
            for side in range(2):
                place = 2 * slot + side
                half = jnp.bitwise_and(jnp.right_shift(part, 16 * side), 65535)
                shift = (place - block % per_tile) * WORD % LANES
                moved = pltpu.roll(half, shift, 1) if shift else half
                riding = jnp.where(quarter == place, moved, riding)
        message_ref[block, tiles * rows :, :] = riding.astype(jnp.float32)


def fit_kernel(history_ref, message_ref, spread_ref, outer_ref, turned_ref, design_ref, stats_ref, *, rows):
    message = message_ref[...]
    clear = read_clear(message, rows, spread_ref)
    values = read_values(message, rows)
    day = lax.broadcasted_iota(jnp.int32, clear.shape, 0)
    weight = jnp.where(day < history_ref[0], clear, 0.0)
    tripled = jnp.dot(outer_ref[...], weight.astype(jnp.bfloat16), preferred_element_type=jnp.float32)
    size = tripled.shape[0] // 3
    normal = tripled[2 * size :] + tripled[size : 2 * size] + tripled[:size]
    seen = [part.astype(jnp.bfloat16) for part in split_rows(weight * values)]
    high, mid, low = [jnp.dot(turned_ref[...], part, preferred_element_type=jnp.float32) for part in seen]
    target = low[:COLS] + mid[COLS : 2 * COLS] + high[2 * COLS :]
    target = target + mid[:COLS] + high[COLS : 2 * COLS]
    target = target + high[:COLS]
    solved = solve_rows(
        lambda i, j: normal[i * (i + 1) // 2 + j][None, :],
        lambda i: target[i][None, :],
    )
    for i in range(COLS):
        stats_ref[i : i + 1, :] = solved[i]
    resid = weight * (values - fit_dot(design_ref, stats_ref[0:COLS, :]))
    squares = jnp.sum(resid * resid, axis=0, keepdims=True)
    count = normal[0:1, :]
    sigma = jnp.sqrt(squares / (count - COLS) + 1e-06)
    stats_ref[COLS : COLS + 1, :] = 1.0 / (sigma * jnp.sqrt(count))
    stats_ref[COLS + 1 :, :] = jnp.zeros_like(stats_ref[COLS + 1 :, :])


def ratio_kernel(start_ref, message_ref, early_ref, stats_ref, spread_ref, design_ref, bounds_ref, out_ref, *, rows):
    message = jnp.concatenate([early_ref[...], message_ref[...]], axis=0)
    clear = read_clear(message, rows, spread_ref)
    values = read_values(message, rows)
    moving = clear * (values - fit_dot(design_ref, stats_ref[0:COLS, :]))
    span = 1
    while span < WINDOW:
        moving = moving + pltpu.roll(moving, span, 0)
        span *= 2
    late = moving.shape[0] - WINDOW
    day = late + lax.broadcasted_iota(jnp.int32, (SUB, late), 1)
    bounds = jnp.broadcast_to(bounds_ref[:, late:].astype(jnp.float32), (SUB, late)) * 0.001
    factor = jnp.transpose(jnp.where(day >= start_ref[0], 1.0 / bounds, 0.0))[:, 0:1]
    ratio = moving[WINDOW:] * stats_ref[COLS : COLS + 1, :] * factor
    blocks = out_ref.shape[0]
    tiles = ratio.shape[1] // LANES
    running = jnp.zeros((1, ratio.shape[1]), jnp.float32)
    for block in range(blocks):
        part = ratio[block * rows : (block + 1) * rows]
        for c in range(tiles):
            at = slice(c * LANES, (c + 1) * LANES)
            out_ref[block, c * rows : (c + 1) * rows, :] = part[:, at]
            out_ref[block, tiles * rows + c : tiles * rows + c + 1, :] = running[:, at]
        running = jnp.maximum(running, jnp.max(jnp.abs(part), axis=0, keepdims=True))


def finish_kernel(upper_ref, message_ref, out_ref, peak_ref):
    blocks, length, _ = message_ref.shape
    rows = out_ref.shape[0]
    tiles = (length - SUB) // rows
    upper = upper_ref[0] > 0
    row = lax.broadcasted_iota(jnp.int32, (rows, LANES), 0)
    for block in range(blocks):
        for c in range(tiles):
            start = (block * tiles + c) * LANES
            ratio = jnp.where(upper, message_ref[block, c * rows : (c + 1) * rows, :], 0.0)
            carry = jnp.where(upper, message_ref[block, tiles * rows + c : tiles * rows + c + 1, :], 0.0)
            peak = jnp.maximum(jnp.abs(ratio), carry)
            span = 1
            while span < rows:
                peak = jnp.maximum(peak, jnp.where(row >= span, pltpu.roll(peak, span, 0), 0.0))
                span *= 2
            out_ref[:, start : start + LANES] = ratio
            peak_ref[:, start : start + LANES] = peak


SMEM = pl.BlockSpec(memory_space=pltpu.SMEM)
VMEM = pl.BlockSpec(memory_space=pltpu.VMEM)


def f32(*shape):
    return jax.ShapeDtypeStruct(shape, jnp.float32)


def per_device(values, cloud_words, history_len, monitor_start, boundary_table, devices):
    rows, pixels = values.shape
    dates = boundary_table.shape[0]
    half = devices // 2
    late = dates // 2
    width = pixels // half
    length = width // LANES * rows + SUB
    groups = [list(range(half)), list(range(half, devices))]
    upward = [(i, i + half) for i in range(half)]
    design = design_table(dates)
    spread = spread_table(width, max(1, rows // SUB))

    def exchange(blocks):
        return lax.all_to_all(blocks, AXES, 0, 0, axis_index_groups=groups, tiled=True)

    step_message = pl.BlockSpec((half // STEPS, length, LANES), lambda i: (i, 0, 0))
    step_pixels = pl.BlockSpec((rows, pixels // STEPS), lambda i: (0, i))
    step_words = pl.BlockSpec((rows, pixels // WORD // STEPS), lambda i: (0, i))
    message = pl.pallas_call(
        pack_kernel,
        grid=(STEPS,),
        out_shape=f32(half, length, LANES),
        in_specs=[step_pixels, step_words],
        out_specs=step_message,
        name="pack",
    )(values, cloud_words)
    own = exchange(message)
    early = lax.ppermute(own[half - WINDOW // rows :], AXES, upward)
    history = design[:late]
    stats = pl.pallas_call(
        functools.partial(fit_kernel, rows=rows),
        out_shape=f32(2 * COLS, width),
        in_specs=[SMEM] + [VMEM] * 5,
        out_specs=VMEM,
        name="fit",
    )(
        history_len,
        own,
        spread,
        np.concatenate(split_table(outer_table(history)), axis=0),
        np.concatenate(split_table(history.T), axis=0),
        six_wide(history),
    )
    stats = lax.ppermute(stats, AXES, upward)
    message = pl.pallas_call(
        functools.partial(ratio_kernel, rows=rows),
        out_shape=f32(half, length, LANES),
        in_specs=[SMEM] + [VMEM] * 6,
        out_specs=VMEM,
        name="ratio",
    )(monitor_start, own, early, stats, spread, six_wide(design[late - WINDOW :]), boundary_table.reshape(1, dates))
    upper = (lax.axis_index(AXES) >= half).astype(jnp.int32).reshape(1)
    return pl.pallas_call(
        finish_kernel,
        grid=(STEPS,),
        out_shape=(f32(rows, pixels), f32(rows, pixels)),
        in_specs=[SMEM, step_message],
        out_specs=(step_pixels, step_pixels),
        name="finish",
    )(upper, exchange(message))


def solution(mesh):
    placed = (P(AXES, None), P(AXES, None), P(), P(), P())
    return jax.shard_map(
        functools.partial(per_device, devices=mesh.size),
        mesh=mesh,
        in_specs=placed,
        out_specs=(P(AXES, None), P(AXES, None)),
        check_vma=False,
    )
```

```python
import functools
import math

import jax
import jax.numpy as jnp
import ml_dtypes
import numpy as np
from jax import lax
from jax.experimental import pallas as pl
from jax.experimental.pallas import tpu as pltpu
from jax.sharding import PartitionSpec as P

PERIOD = 46
HARMONICS = 3
COLS = 8
WINDOW = 64
WORD = 32
LANES = 128
SUB = 8
STEPS = 4
AXES = ("wide", "narrow")


def design_table(dates):
    day = np.arange(dates).astype(np.float32)
    columns = [np.ones((dates,), np.float32), day / np.float32(dates)]
    for harmonic in range(1, HARMONICS + 1):
        phases = (np.float32(2.0 * math.pi * harmonic / PERIOD) * day).astype(np.float64)
        columns.append(np.cos(phases).astype(np.float32))
        columns.append(np.sin(phases).astype(np.float32))
    return np.stack(columns, axis=1)


def outer_table(design):
    rows = [design[:, i] * design[:, j] for i in range(COLS) for j in range(i + 1)]
    while len(rows) % SUB:
        rows.append(np.zeros_like(rows[0]))
    return np.stack(rows, axis=0)


def split_table(table):
    parts = []
    rest = table
    for _ in range(3):
        part = rest.astype(ml_dtypes.bfloat16)
        parts.append(part)
        rest = rest - part.astype(np.float32)
    return parts


def split_rows(array):
    high = array.astype(jnp.bfloat16).astype(jnp.float32)
    rest = array - high
    mid = rest.astype(jnp.bfloat16).astype(jnp.float32)
    return high, mid, rest - mid


def spread_table(pixels, slots):
    pixel = np.arange(pixels)
    byte = (pixel % WORD) // 8
    table = np.zeros((slots, 2 * LANES, pixels), np.float32)
    for slot in range(slots):
        table[slot, (byte % 2) * LANES + 64 * slot + 32 * (byte // 2) + pixel // WORD, pixel] = 1.0
    return table.astype(ml_dtypes.bfloat16)


def flat_rows(blocks):
    count, rows, lanes = blocks.shape
    if rows % SUB == 0:
        return blocks.reshape(count * rows, lanes)
    return jnp.concatenate([blocks[i] for i in range(count)], axis=0)


def read_values(message, rows):
    tiles = (message.shape[1] - SUB) // rows
    return jnp.concatenate([flat_rows(message[:, c * rows : (c + 1) * rows]) for c in range(tiles)], axis=1)


def read_clear(message, rows, spread_ref):
    blocks = message.shape[0]
    halves = message[:, -SUB:].reshape(blocks * SUB, LANES).astype(jnp.int32)
    planes = [jnp.bitwise_and(halves, 255), jnp.right_shift(halves, 8)]
    planes = jnp.concatenate([plane.astype(jnp.float32) for plane in planes], axis=1).astype(jnp.bfloat16)
    found = []
    for slot in range(spread_ref.shape[0]):
        byte = jnp.dot(planes, spread_ref[slot], preferred_element_type=jnp.float32).astype(jnp.int32)
        bit = jnp.bitwise_and(lax.broadcasted_iota(jnp.int32, byte.shape, 1), 7)
        flags = jnp.bitwise_and(jnp.right_shift(byte, bit), 1).astype(jnp.float32)
        found.append(flags.reshape(blocks, SUB, -1)[:, : min(rows, SUB)])
    return flat_rows(jnp.concatenate(found, axis=1))


def fit_dot(design_ref, coeffs):
    high, mid, low = split_rows(coeffs)
    stacked = jnp.concatenate([high, high, high, mid, mid, low], axis=0).astype(jnp.bfloat16)
    return jnp.dot(design_ref[...], stacked, preferred_element_type=jnp.float32)


def six_wide(design):
    high, mid, low = split_table(design)
    return np.concatenate([high, mid, low, high, mid, high], axis=1)


def solve_rows(normal, target):
    factor = {}
    inverse = []
    for col in range(COLS):
        for row in range(col, COLS):
            summed = normal(row, col)
            for mid in range(col):
                summed = summed - factor[row, mid] * factor[col, mid]
            if row == col:
                inverse.append(1.0 / jnp.sqrt(summed))
            else:
                factor[row, col] = summed * inverse[col]
    forward = []
    for row in range(COLS):
        summed = target(row)
        for mid in range(row):
            summed = summed - factor[row, mid] * forward[mid]
        forward.append(summed * inverse[row])
    solved = [None] * COLS
    for row in reversed(range(COLS)):
        summed = forward[row]
        for mid in range(row + 1, COLS):
            summed = summed - factor[mid, row] * solved[mid]
        solved[row] = summed * inverse[row]
    return solved


def pack_kernel(values_ref, words_ref, message_ref):
    rows = values_ref.shape[0]
    blocks, length, _ = message_ref.shape
    tiles = (length - SUB) // rows
    for block in range(blocks):
        for c in range(tiles):
            start = (block * tiles + c) * LANES
            message_ref[block, c * rows : (c + 1) * rows, :] = values_ref[:, start : start + LANES]
        per_tile = LANES // WORD
        words = words_ref[:, block // per_tile * LANES : (block // per_tile + 1) * LANES]
        if rows % SUB:
            words = jnp.concatenate([words, jnp.zeros((SUB - rows % SUB, LANES), jnp.int32)], axis=0)
        quarter = lax.broadcasted_iota(jnp.int32, (SUB, LANES), 1) // WORD
        riding = jnp.zeros((SUB, LANES), jnp.int32)
        for slot in range(words.shape[0] // SUB):
            part = words[slot * SUB : (slot + 1) * SUB]
            for side in range(2):
                place = 2 * slot + side
                half = jnp.bitwise_and(jnp.right_shift(part, 16 * side), 65535)
                shift = (place - block % per_tile) * WORD % LANES
                moved = pltpu.roll(half, shift, 1) if shift else half
                riding = jnp.where(quarter == place, moved, riding)
        message_ref[block, tiles * rows :, :] = riding.astype(jnp.float32)


def fit_kernel(history_ref, message_ref, spread_ref, outer_ref, turned_ref, design_ref, stats_ref, values_ref, clear_ref, *, rows):
    message = message_ref[...]
    clear = read_clear(message, rows, spread_ref)
    values = read_values(message, rows)
    values_ref[...] = values
    clear_ref[...] = clear
    day = lax.broadcasted_iota(jnp.int32, clear.shape, 0)
    weight = jnp.where(day < history_ref[0], clear, 0.0)
    tripled = jnp.dot(outer_ref[...], weight.astype(jnp.bfloat16), preferred_element_type=jnp.float32)
    size = tripled.shape[0] // 3
    normal = tripled[2 * size :] + tripled[size : 2 * size] + tripled[:size]
    seen = [part.astype(jnp.bfloat16) for part in split_rows(weight * values)]
    high, mid, low = [jnp.dot(turned_ref[...], part, preferred_element_type=jnp.float32) for part in seen]
    target = low[:COLS] + mid[COLS : 2 * COLS] + high[2 * COLS :]
    target = target + mid[:COLS] + high[COLS : 2 * COLS]
    target = target + high[:COLS]
    solved = solve_rows(
        lambda i, j: normal[i * (i + 1) // 2 + j][None, :],
        lambda i: target[i][None, :],
    )
    resid = weight * (values - fit_dot(design_ref, jnp.concatenate(solved, axis=0)))
    squares = jnp.sum(resid * resid, axis=0, keepdims=True)
    count = normal[0:1, :]
    sigma = jnp.sqrt(squares / (count - COLS) + 1e-06)
    tiles = count.shape[1] // LANES
    for i, stat in enumerate(solved + [1.0 / (sigma * jnp.sqrt(count))]):
        for c in range(tiles):
            stats_ref[i * tiles + c : i * tiles + c + 1, :] = stat[:, c * LANES : (c + 1) * LANES]


def ratio_kernel(start_ref, values_ref, clear_ref, early_ref, stats_ref, spread_ref, design_ref, bounds_ref, out_ref, *, rows):
    tiles = stats_ref.shape[0] // (COLS + 1)
    early = early_ref[...]
    clear = jnp.concatenate([read_clear(early, rows, spread_ref), clear_ref[...]], axis=0)
    values = jnp.concatenate([read_values(early, rows), values_ref[...]], axis=0)
    stat_rows = [stats_ref[pl.ds(c, COLS + 1, stride=tiles), :] for c in range(tiles)]
    coeffs = jnp.concatenate([stat[:COLS] for stat in stat_rows], axis=1)
    scale = jnp.concatenate([stat[COLS:] for stat in stat_rows], axis=1)
    moving = clear * (values - fit_dot(design_ref, coeffs))
    span = 1
    while span < WINDOW:
        moving = moving + pltpu.roll(moving, span, 0)
        span *= 2
    late = moving.shape[0] - WINDOW
    day = late + lax.broadcasted_iota(jnp.int32, (SUB, late), 1)
    bounds = jnp.broadcast_to(bounds_ref[:, late:].astype(jnp.float32), (SUB, late)) * 0.001
    factor = jnp.transpose(jnp.where(day >= start_ref[0], 1.0 / bounds, 0.0))[:, 0:1]
    ratio = moving[WINDOW:] * scale * factor
    blocks = out_ref.shape[0]
    running = jnp.zeros((1, ratio.shape[1]), jnp.float32)
    for block in range(blocks):
        part = ratio[block * rows : (block + 1) * rows]
        for c in range(tiles):
            at = slice(c * LANES, (c + 1) * LANES)
            out_ref[block, c * rows : (c + 1) * rows, :] = part[:, at]
            out_ref[block, tiles * rows + c : tiles * rows + c + 1, :] = running[:, at]
        running = jnp.maximum(running, jnp.max(jnp.abs(part), axis=0, keepdims=True))


def finish_kernel(upper_ref, message_ref, out_ref, peak_ref):
    _, length, _ = message_ref.shape
    rows, lanes = out_ref.shape
    tiles = (length - SUB) // rows
    blocks = lanes // (tiles * LANES)
    first = pl.program_id(0) * blocks
    upper = upper_ref[0] > 0
    row = lax.broadcasted_iota(jnp.int32, (rows, LANES), 0)
    for block in range(blocks):
        for c in range(tiles):
            start = (block * tiles + c) * LANES
            ratio = jnp.where(upper, message_ref[first + block, c * rows : (c + 1) * rows, :], 0.0)
            carry = jnp.where(upper, message_ref[first + block, tiles * rows + c : tiles * rows + c + 1, :], 0.0)
            peak = jnp.maximum(jnp.abs(ratio), carry)
            span = 1
            while span < rows:
                peak = jnp.maximum(peak, jnp.where(row >= span, pltpu.roll(peak, span, 0), 0.0))
                span *= 2
            out_ref[:, start : start + LANES] = ratio
            peak_ref[:, start : start + LANES] = peak


SMEM = pl.BlockSpec(memory_space=pltpu.SMEM)
GRANT = pltpu.CompilerParams(vmem_limit_bytes=24 << 20)
VMEM = pl.BlockSpec(memory_space=pltpu.VMEM)


def f32(*shape):
    return jax.ShapeDtypeStruct(shape, jnp.float32)


def per_device(values, cloud_words, history_len, monitor_start, boundary_table, devices):
    rows, pixels = values.shape
    dates = boundary_table.shape[0]
    half = devices // 2
    late = dates // 2
    width = pixels // half
    length = width // LANES * rows + SUB
    groups = [list(range(half)), list(range(half, devices))]
    upward = [(i, i + half) for i in range(half)]
    design = design_table(dates)
    spread = spread_table(width, max(1, rows // SUB))

    def exchange(blocks):
        return lax.all_to_all(blocks, AXES, 0, 0, axis_index_groups=groups, tiled=True)

    step_message = pl.BlockSpec((half // STEPS, length, LANES), lambda i: (i, 0, 0))
    step_pixels = pl.BlockSpec((rows, pixels // STEPS), lambda i: (0, i))
    step_words = pl.BlockSpec((rows, pixels // WORD // STEPS), lambda i: (0, i))
    message = pl.pallas_call(
        pack_kernel,
        grid=(STEPS,),
        out_shape=f32(half, length, LANES),
        in_specs=[step_pixels, step_words],
        out_specs=step_message,
        compiler_params=GRANT,
        name="pack",
    )(values, cloud_words)
    own = exchange(message)
    early = lax.ppermute(own[half - WINDOW // rows :], AXES, upward)
    history = design[:late]
    stats, values, clear = pl.pallas_call(
        functools.partial(fit_kernel, rows=rows),
        out_shape=(f32((COLS + 1) * (width // LANES), LANES), f32(late, width), f32(late, width)),
        in_specs=[SMEM] + [VMEM] * 5,
        out_specs=(VMEM, VMEM, VMEM),
        compiler_params=GRANT,
        name="fit",
    )(
        history_len,
        own,
        spread,
        np.concatenate(split_table(outer_table(history)), axis=0),
        np.concatenate(split_table(history.T), axis=0),
        six_wide(history),
    )
    stats = lax.ppermute(stats, AXES, upward)
    message = pl.pallas_call(
        functools.partial(ratio_kernel, rows=rows),
        out_shape=f32(half, length, LANES),
        in_specs=[SMEM] + [VMEM] * 7,
        out_specs=VMEM,
        compiler_params=GRANT,
        name="ratio",
    )(monitor_start, values, clear, early, stats, spread, six_wide(design[late - WINDOW :]), boundary_table.reshape(1, dates))
    upper = (lax.axis_index(AXES) >= half).astype(jnp.int32).reshape(1)
    return pl.pallas_call(
        finish_kernel,
        grid=(STEPS,),
        out_shape=(f32(rows, pixels), f32(rows, pixels)),
        in_specs=[SMEM, VMEM],
        out_specs=(step_pixels, step_pixels),
        compiler_params=GRANT,
        name="finish",
    )(upper, exchange(message))


def solution(mesh):
    placed = (P(AXES, None), P(AXES, None), P(), P(), P())
    return jax.shard_map(
        functools.partial(per_device, devices=mesh.size),
        mesh=mesh,
        in_specs=placed,
        out_specs=(P(AXES, None), P(AXES, None)),
        check_vma=False,
    )
```

```python
import functools
import math

import jax
import jax.numpy as jnp
import ml_dtypes
import numpy as np
from jax import lax
from jax.experimental import pallas as pl
from jax.experimental.pallas import tpu as pltpu
from jax.sharding import PartitionSpec as P

PERIOD = 46
HARMONICS = 3
COLS = 8
WINDOW = 64
WORD = 32
LANES = 128
SUB = 8
STEPS = 4
AXES = ("wide", "narrow")


def design_table(dates):
    day = np.arange(dates).astype(np.float32)
    columns = [np.ones((dates,), np.float32), day / np.float32(dates)]
    for harmonic in range(1, HARMONICS + 1):
        phases = (np.float32(2.0 * math.pi * harmonic / PERIOD) * day).astype(np.float64)
        columns.append(np.cos(phases).astype(np.float32))
        columns.append(np.sin(phases).astype(np.float32))
    return np.stack(columns, axis=1)


def outer_table(design):
    rows = [design[:, i] * design[:, j] for i in range(COLS) for j in range(i + 1)]
    while len(rows) % SUB:
        rows.append(np.zeros_like(rows[0]))
    return np.stack(rows, axis=0)


def split_table(table):
    parts = []
    rest = table
    for _ in range(3):
        part = rest.astype(ml_dtypes.bfloat16)
        parts.append(part)
        rest = rest - part.astype(np.float32)
    return parts


def split_rows(array):
    high = array.astype(jnp.bfloat16).astype(jnp.float32)
    rest = array - high
    mid = rest.astype(jnp.bfloat16).astype(jnp.float32)
    return high, mid, rest - mid


def spread_table(pixels, slots):
    pixel = np.arange(pixels)
    byte = (pixel % WORD) // 8
    table = np.zeros((slots, 2 * LANES, pixels), np.float32)
    for slot in range(slots):
        table[slot, (byte % 2) * LANES + 64 * slot + 32 * (byte // 2) + pixel // WORD, pixel] = 1.0
    return table.astype(ml_dtypes.bfloat16)


def flat_rows(blocks):
    count, rows, lanes = blocks.shape
    if rows % SUB == 0:
        return blocks.reshape(count * rows, lanes)
    return jnp.concatenate([blocks[i] for i in range(count)], axis=0)


def read_values(message, rows):
    tiles = (message.shape[1] - SUB) // rows
    return jnp.concatenate([flat_rows(message[:, c * rows : (c + 1) * rows]) for c in range(tiles)], axis=1)


def read_clear(message, rows, spread_ref):
    blocks = message.shape[0]
    halves = message[:, -SUB:].reshape(blocks * SUB, LANES).astype(jnp.int32)
    planes = [jnp.bitwise_and(halves, 255), jnp.right_shift(halves, 8)]
    planes = jnp.concatenate([plane.astype(jnp.float32) for plane in planes], axis=1).astype(jnp.bfloat16)
    found = []
    for slot in range(spread_ref.shape[0]):
        byte = jnp.dot(planes, spread_ref[slot], preferred_element_type=jnp.float32).astype(jnp.int32)
        bit = jnp.bitwise_and(lax.broadcasted_iota(jnp.int32, byte.shape, 1), 7)
        flags = jnp.bitwise_and(jnp.right_shift(byte, bit), 1).astype(jnp.float32)
        found.append(flags.reshape(blocks, SUB, -1)[:, : min(rows, SUB)])
    return flat_rows(jnp.concatenate(found, axis=1))


def fit_dot(design_ref, coeffs):
    high, mid, low = split_rows(coeffs)
    stacked = jnp.concatenate([high, high, high, mid, mid, low], axis=0).astype(jnp.bfloat16)
    return jnp.dot(design_ref[...], stacked, preferred_element_type=jnp.float32)


def six_wide(design):
    high, mid, low = split_table(design)
    return np.concatenate([high, mid, low, high, mid, high], axis=1)


def solve_rows(normal, target):
    factor = {}
    inverse = []
    for col in range(COLS):
        for row in range(col, COLS):
            summed = normal(row, col)
            for mid in range(col):
                summed = summed - factor[row, mid] * factor[col, mid]
            if row == col:
                inverse.append(1.0 / jnp.sqrt(summed))
            else:
                factor[row, col] = summed * inverse[col]
    forward = []
    for row in range(COLS):
        summed = target(row)
        for mid in range(row):
            summed = summed - factor[row, mid] * forward[mid]
        forward.append(summed * inverse[row])
    solved = [None] * COLS
    for row in reversed(range(COLS)):
        summed = forward[row]
        for mid in range(row + 1, COLS):
            summed = summed - factor[mid, row] * solved[mid]
        solved[row] = summed * inverse[row]
    return solved


def pack_kernel(values_ref, words_ref, message_ref):
    rows = values_ref.shape[0]
    blocks, length, _ = message_ref.shape
    tiles = (length - SUB) // rows
    for block in range(blocks):
        for c in range(tiles):
            start = (block * tiles + c) * LANES
            message_ref[block, c * rows : (c + 1) * rows, :] = values_ref[:, start : start + LANES]
        per_tile = LANES // WORD
        words = words_ref[:, block // per_tile * LANES : (block // per_tile + 1) * LANES]
        if rows % SUB:
            words = jnp.concatenate([words, jnp.zeros((SUB - rows % SUB, LANES), jnp.int32)], axis=0)
        quarter = lax.broadcasted_iota(jnp.int32, (SUB, LANES), 1) // WORD
        riding = jnp.zeros((SUB, LANES), jnp.int32)
        for slot in range(words.shape[0] // SUB):
            part = words[slot * SUB : (slot + 1) * SUB]
            for side in range(2):
                place = 2 * slot + side
                half = jnp.bitwise_and(jnp.right_shift(part, 16 * side), 65535)
                shift = (place - block % per_tile) * WORD % LANES
                moved = pltpu.roll(half, shift, 1) if shift else half
                riding = jnp.where(quarter == place, moved, riding)
        message_ref[block, tiles * rows :, :] = riding.astype(jnp.float32)


def fit_kernel(history_ref, message_ref, spread_ref, outer_ref, turned_ref, design_ref, stats_ref, seen_ref, *, rows):
    message = message_ref[...]
    clear = read_clear(message, rows, spread_ref)
    values = read_values(message, rows)
    seen_ref[: values.shape[0]] = values
    seen_ref[values.shape[0] :] = clear
    day = lax.broadcasted_iota(jnp.int32, clear.shape, 0)
    weight = jnp.where(day < history_ref[0], clear, 0.0)
    tripled = jnp.dot(outer_ref[...], weight.astype(jnp.bfloat16), preferred_element_type=jnp.float32)
    size = tripled.shape[0] // 3
    normal = tripled[2 * size :] + tripled[size : 2 * size] + tripled[:size]
    seen = [part.astype(jnp.bfloat16) for part in split_rows(weight * values)]
    high, mid, low = [jnp.dot(turned_ref[...], part, preferred_element_type=jnp.float32) for part in seen]
    target = low[:COLS] + mid[COLS : 2 * COLS] + high[2 * COLS :]
    target = target + mid[:COLS] + high[COLS : 2 * COLS]
    target = target + high[:COLS]
    solved = solve_rows(
        lambda i, j: normal[i * (i + 1) // 2 + j][None, :],
        lambda i: target[i][None, :],
    )
    resid = weight * (values - fit_dot(design_ref, jnp.concatenate(solved, axis=0)))
    squares = jnp.sum(resid * resid, axis=0, keepdims=True)
    count = normal[0:1, :]
    sigma = jnp.sqrt(squares / (count - COLS) + 1e-06)
    tiles = count.shape[1] // LANES
    for i, stat in enumerate(solved + [1.0 / (sigma * jnp.sqrt(count))]):
        for c in range(tiles):
            stats_ref[i * tiles + c : i * tiles + c + 1, :] = stat[:, c * LANES : (c + 1) * LANES]
    blocks, length, _ = message.shape
    for i in range(WINDOW // rows):
        start = (COLS + 1) * tiles + i * length
        stats_ref[start : start + length, :] = message_ref[blocks - 1 - i]


def ratio_kernel(start_ref, seen_ref, stats_ref, spread_ref, design_ref, bounds_ref, out_ref, *, rows):
    late = seen_ref.shape[0] // 2
    tiles = seen_ref.shape[1] // LANES
    length = tiles * rows + SUB
    starts = [(COLS + 1) * tiles + i * length for i in reversed(range(WINDOW // rows))]
    early = jnp.concatenate([stats_ref[start : start + length, :][None] for start in starts], axis=0)
    clear = jnp.concatenate([read_clear(early, rows, spread_ref), seen_ref[late:]], axis=0)
    values = jnp.concatenate([read_values(early, rows), seen_ref[:late]], axis=0)
    stat_rows = [stats_ref[pl.ds(c, COLS + 1, stride=tiles), :] for c in range(tiles)]
    coeffs = jnp.concatenate([stat[:COLS] for stat in stat_rows], axis=1)
    scale = jnp.concatenate([stat[COLS:] for stat in stat_rows], axis=1)
    moving = clear * (values - fit_dot(design_ref, coeffs))
    span = 1
    while span < WINDOW:
        moving = moving + pltpu.roll(moving, span, 0)
        span *= 2
    day = late + lax.broadcasted_iota(jnp.int32, (SUB, late), 1)
    bounds = jnp.broadcast_to(bounds_ref[:, late:].astype(jnp.float32), (SUB, late)) * 0.001
    factor = jnp.transpose(jnp.where(day >= start_ref[0], 1.0 / bounds, 0.0))[:, 0:1]
    ratio = moving[WINDOW:] * scale * factor
    blocks = out_ref.shape[0]
    running = jnp.zeros((1, ratio.shape[1]), jnp.float32)
    for block in range(blocks):
        part = ratio[block * rows : (block + 1) * rows]
        for c in range(tiles):
            at = slice(c * LANES, (c + 1) * LANES)
            out_ref[block, c * rows : (c + 1) * rows, :] = part[:, at]
            out_ref[block, tiles * rows + c : tiles * rows + c + 1, :] = running[:, at]
        running = jnp.maximum(running, jnp.max(jnp.abs(part), axis=0, keepdims=True))


def finish_kernel(upper_ref, message_ref, out_ref, peak_ref):
    _, length, _ = message_ref.shape
    rows, lanes = out_ref.shape
    tiles = (length - SUB) // rows
    blocks = lanes // (tiles * LANES)
    first = pl.program_id(0) * blocks
    upper = upper_ref[0] > 0
    row = lax.broadcasted_iota(jnp.int32, (rows, LANES), 0)
    for block in range(blocks):
        for c in range(tiles):
            start = (block * tiles + c) * LANES
            ratio = jnp.where(upper, message_ref[first + block, c * rows : (c + 1) * rows, :], 0.0)
            carry = jnp.where(upper, message_ref[first + block, tiles * rows + c : tiles * rows + c + 1, :], 0.0)
            peak = jnp.maximum(jnp.abs(ratio), carry)
            span = 1
            while span < rows:
                peak = jnp.maximum(peak, jnp.where(row >= span, pltpu.roll(peak, span, 0), 0.0))
                span *= 2
            out_ref[:, start : start + LANES] = ratio
            peak_ref[:, start : start + LANES] = peak


SMEM = pl.BlockSpec(memory_space=pltpu.SMEM)
GRANT = pltpu.CompilerParams(vmem_limit_bytes=12 << 20)
VMEM = pl.BlockSpec(memory_space=pltpu.VMEM)


def f32(*shape):
    return jax.ShapeDtypeStruct(shape, jnp.float32)


def per_device(values, cloud_words, history_len, monitor_start, boundary_table, devices):
    rows, pixels = values.shape
    dates = boundary_table.shape[0]
    half = devices // 2
    late = dates // 2
    width = pixels // half
    length = width // LANES * rows + SUB
    groups = [list(range(half)), list(range(half, devices))]
    upward = [(i, i + half) for i in range(half)]
    design = design_table(dates)
    spread = spread_table(width, max(1, rows // SUB))

    def exchange(blocks):
        return lax.all_to_all(blocks, AXES, 0, 0, axis_index_groups=groups, tiled=True)

    step_message = pl.BlockSpec((half // STEPS, length, LANES), lambda i: (i, 0, 0))
    step_pixels = pl.BlockSpec((rows, pixels // STEPS), lambda i: (0, i))
    step_words = pl.BlockSpec((rows, pixels // WORD // STEPS), lambda i: (0, i))
    message = pl.pallas_call(
        pack_kernel,
        grid=(STEPS,),
        out_shape=f32(half, length, LANES),
        in_specs=[step_pixels, step_words],
        out_specs=step_message,
        compiler_params=GRANT,
        name="pack",
    )(values, cloud_words)
    own = exchange(message)
    history = design[:late]
    base = (COLS + 1) * (width // LANES)
    stats, seen = pl.pallas_call(
        functools.partial(fit_kernel, rows=rows),
        out_shape=(f32(base + WINDOW // rows * length, LANES), f32(2 * late, width)),
        in_specs=[SMEM] + [VMEM] * 5,
        out_specs=(VMEM, VMEM),
        compiler_params=GRANT,
        name="fit",
    )(
        history_len,
        own,
        spread,
        np.concatenate(split_table(outer_table(history)), axis=0),
        np.concatenate(split_table(history.T), axis=0),
        six_wide(history),
    )
    piece = WINDOW // rows // STEPS * length

    def send(count):
        def branch(array):
            got = lax.ppermute(array[: base + count * piece], AXES, upward)
            return lax.dynamic_update_slice(array, got, (0, 0))

        return branch

    reach = jnp.maximum(late + WINDOW - 1 - monitor_start[0], 0)
    stats = lax.switch((reach * STEPS + WINDOW - 1) // WINDOW, [send(count) for count in range(STEPS + 1)], stats)
    message = pl.pallas_call(
        functools.partial(ratio_kernel, rows=rows),
        out_shape=f32(half, length, LANES),
        in_specs=[SMEM] + [VMEM] * 5,
        out_specs=VMEM,
        compiler_params=GRANT,
        name="ratio",
    )(monitor_start, seen, stats, spread, six_wide(design[late - WINDOW :]), boundary_table.reshape(1, dates))
    upper = (lax.axis_index(AXES) >= half).astype(jnp.int32).reshape(1)
    return pl.pallas_call(
        finish_kernel,
        grid=(STEPS,),
        out_shape=(f32(rows, pixels), f32(rows, pixels)),
        in_specs=[SMEM, VMEM],
        out_specs=(step_pixels, step_pixels),
        compiler_params=GRANT,
        name="finish",
    )(upper, exchange(message))


def solution(mesh):
    placed = (P(AXES, None), P(AXES, None), P(), P(), P())
    return jax.shard_map(
        functools.partial(per_device, devices=mesh.size),
        mesh=mesh,
        in_specs=placed,
        out_specs=(P(AXES, None), P(AXES, None)),
        check_vma=False,
    )
```

```python
import functools
import math

import jax
import jax.numpy as jnp
import ml_dtypes
import numpy as np
from jax import lax
from jax.experimental import pallas as pl
from jax.experimental.pallas import tpu as pltpu
from jax.sharding import PartitionSpec as P

PERIOD = 46
HARMONICS = 3
COLS = 8
WINDOW = 64
WORD = 32
LANES = 128
SUB = 8
STEPS = 4
AXES = ("wide", "narrow")


def design_table(dates):
    day = np.arange(dates).astype(np.float32)
    columns = [np.ones((dates,), np.float32), day / np.float32(dates)]
    for harmonic in range(1, HARMONICS + 1):
        phases = (np.float32(2.0 * math.pi * harmonic / PERIOD) * day).astype(np.float64)
        columns.append(np.cos(phases).astype(np.float32))
        columns.append(np.sin(phases).astype(np.float32))
    return np.stack(columns, axis=1)


def outer_table(design):
    rows = [design[:, i] * design[:, j] for i in range(COLS) for j in range(i + 1)]
    while len(rows) % SUB:
        rows.append(np.zeros_like(rows[0]))
    return np.stack(rows, axis=0)


def split_table(table):
    parts = []
    rest = table
    for _ in range(3):
        part = rest.astype(ml_dtypes.bfloat16)
        parts.append(part)
        rest = rest - part.astype(np.float32)
    return parts


def split_rows(array):
    high = array.astype(jnp.bfloat16).astype(jnp.float32)
    rest = array - high
    mid = rest.astype(jnp.bfloat16).astype(jnp.float32)
    return high, mid, rest - mid


def spread_table(pixels, slots):
    pixel = np.arange(pixels)
    byte = (pixel % WORD) // 8
    table = np.zeros((slots, 2 * LANES, pixels), np.float32)
    for slot in range(slots):
        table[slot, (byte % 2) * LANES + 64 * slot + 32 * (byte // 2) + pixel // WORD, pixel] = 1.0
    return table.astype(ml_dtypes.bfloat16)


def flat_rows(blocks):
    count, rows, lanes = blocks.shape
    if rows % SUB == 0:
        return blocks.reshape(count * rows, lanes)
    return jnp.concatenate([blocks[i] for i in range(count)], axis=0)


def read_values(message, rows):
    tiles = (message.shape[1] - SUB) // rows
    return jnp.concatenate([flat_rows(message[:, c * rows : (c + 1) * rows]) for c in range(tiles)], axis=1)


def read_clear(message, rows, spread_ref):
    blocks = message.shape[0]
    halves = message[:, -SUB:].reshape(blocks * SUB, LANES).astype(jnp.int32)
    planes = [jnp.bitwise_and(halves, 255), jnp.right_shift(halves, 8)]
    planes = jnp.concatenate([plane.astype(jnp.float32) for plane in planes], axis=1).astype(jnp.bfloat16)
    found = []
    for slot in range(spread_ref.shape[0]):
        byte = jnp.dot(planes, spread_ref[slot], preferred_element_type=jnp.float32).astype(jnp.int32)
        bit = jnp.bitwise_and(lax.broadcasted_iota(jnp.int32, byte.shape, 1), 7)
        flags = jnp.bitwise_and(jnp.right_shift(byte, bit), 1).astype(jnp.float32)
        found.append(flags.reshape(blocks, SUB, -1)[:, : min(rows, SUB)])
    return flat_rows(jnp.concatenate(found, axis=1))


def fit_dot(design_ref, coeffs):
    high, mid, low = split_rows(coeffs)
    stacked = jnp.concatenate([high, high, high, mid, mid, low], axis=0).astype(jnp.bfloat16)
    return jnp.dot(design_ref[...], stacked, preferred_element_type=jnp.float32)


def six_wide(design):
    high, mid, low = split_table(design)
    return np.concatenate([high, mid, low, high, mid, high], axis=1)


def solve_rows(normal, target):
    factor = {}
    inverse = []
    for col in range(COLS):
        for row in range(col, COLS):
            summed = normal(row, col)
            for mid in range(col):
                summed = summed - factor[row, mid] * factor[col, mid]
            if row == col:
                inverse.append(1.0 / jnp.sqrt(summed))
            else:
                factor[row, col] = summed * inverse[col]
    forward = []
    for row in range(COLS):
        summed = target(row)
        for mid in range(row):
            summed = summed - factor[row, mid] * forward[mid]
        forward.append(summed * inverse[row])
    solved = [None] * COLS
    for row in reversed(range(COLS)):
        summed = forward[row]
        for mid in range(row + 1, COLS):
            summed = summed - factor[mid, row] * solved[mid]
        solved[row] = summed * inverse[row]
    return solved


def pack_kernel(values_ref, words_ref, message_ref):
    rows = values_ref.shape[0]
    blocks, length, _ = message_ref.shape
    tiles = (length - SUB) // rows
    for block in range(blocks):
        for c in range(tiles):
            start = (block * tiles + c) * LANES
            message_ref[block, c * rows : (c + 1) * rows, :] = values_ref[:, start : start + LANES]
        per_tile = LANES // WORD
        words = words_ref[:, block // per_tile * LANES : (block // per_tile + 1) * LANES]
        if rows % SUB:
            words = jnp.concatenate([words, jnp.zeros((SUB - rows % SUB, LANES), jnp.int32)], axis=0)
        quarter = lax.broadcasted_iota(jnp.int32, (SUB, LANES), 1) // WORD
        riding = jnp.zeros((SUB, LANES), jnp.int32)
        for slot in range(words.shape[0] // SUB):
            part = words[slot * SUB : (slot + 1) * SUB]
            for side in range(2):
                place = 2 * slot + side
                half = jnp.bitwise_and(jnp.right_shift(part, 16 * side), 65535)
                shift = (place - block % per_tile) * WORD % LANES
                moved = pltpu.roll(half, shift, 1) if shift else half
                riding = jnp.where(quarter == place, moved, riding)
        message_ref[block, tiles * rows :, :] = riding.astype(jnp.float32)


def fit_kernel(history_ref, message_ref, spread_ref, outer_ref, turned_ref, design_ref, stats_ref, seen_ref, *, rows):
    message = message_ref[...]
    clear = read_clear(message, rows, spread_ref)
    values = read_values(message, rows)
    seen_ref[: values.shape[0]] = values
    seen_ref[values.shape[0] :] = clear
    day = lax.broadcasted_iota(jnp.int32, clear.shape, 0)
    weight = jnp.where(day < history_ref[0], clear, 0.0)
    tripled = jnp.dot(outer_ref[...], weight.astype(jnp.bfloat16), preferred_element_type=jnp.float32)
    size = tripled.shape[0] // 3
    normal = tripled[2 * size :] + tripled[size : 2 * size] + tripled[:size]
    seen = [part.astype(jnp.bfloat16) for part in split_rows(weight * values)]
    high, mid, low = [jnp.dot(turned_ref[...], part, preferred_element_type=jnp.float32) for part in seen]
    target = low[:COLS] + mid[COLS : 2 * COLS] + high[2 * COLS :]
    target = target + mid[:COLS] + high[COLS : 2 * COLS]
    target = target + high[:COLS]
    solved = solve_rows(
        lambda i, j: normal[i * (i + 1) // 2 + j][None, :],
        lambda i: target[i][None, :],
    )
    resid = weight * (values - fit_dot(design_ref, jnp.concatenate(solved, axis=0)))
    squares = jnp.sum(resid * resid, axis=0, keepdims=True)
    count = normal[0:1, :]
    sigma = jnp.sqrt(squares / (count - COLS) + 1e-06)
    tiles = count.shape[1] // LANES
    for i, stat in enumerate(solved + [1.0 / (sigma * jnp.sqrt(count))]):
        for c in range(tiles):
            stats_ref[i * tiles + c : i * tiles + c + 1, :] = stat[:, c * LANES : (c + 1) * LANES]
    blocks, length, _ = message.shape
    for i in range(WINDOW // rows):
        start = (COLS + 1) * tiles + i * length
        stats_ref[start : start + length, :] = message_ref[blocks - 1 - i]


def ratio_kernel(start_ref, seen_ref, stats_ref, spread_ref, design_ref, bounds_ref, out_ref, *, rows):
    late = seen_ref.shape[0] // 2
    tiles = seen_ref.shape[1] // LANES
    length = tiles * rows + SUB
    base = (COLS + 1) * tiles
    starts = [base + i * length for i in reversed(range((stats_ref.shape[0] - base) // length))]
    clear = seen_ref[late:]
    values = seen_ref[:late]
    absent = WINDOW - len(starts) * rows
    if starts:
        early = jnp.concatenate([stats_ref[start : start + length, :][None] for start in starts], axis=0)
        clear = jnp.concatenate([read_clear(early, rows, spread_ref), clear], axis=0)
        values = jnp.concatenate([read_values(early, rows), values], axis=0)
    stat_rows = [stats_ref[pl.ds(c, COLS + 1, stride=tiles), :] for c in range(tiles)]
    coeffs = jnp.concatenate([stat[:COLS] for stat in stat_rows], axis=1)
    scale = jnp.concatenate([stat[COLS:] for stat in stat_rows], axis=1)
    moving = clear * (values - fit_dot(design_ref.at[absent:], coeffs))
    if absent:
        moving = jnp.concatenate([jnp.zeros((absent, moving.shape[1]), jnp.float32), moving], axis=0)
    span = 1
    while span < WINDOW:
        moving = moving + pltpu.roll(moving, span, 0)
        span *= 2
    day = late + lax.broadcasted_iota(jnp.int32, (SUB, late), 1)
    bounds = jnp.broadcast_to(bounds_ref[:, late:].astype(jnp.float32), (SUB, late)) * 0.001
    factor = jnp.transpose(jnp.where(day >= start_ref[0], 1.0 / bounds, 0.0))[:, 0:1]
    ratio = moving[WINDOW:] * scale * factor
    blocks = out_ref.shape[0]
    running = jnp.zeros((1, ratio.shape[1]), jnp.float32)
    for block in range(blocks):
        part = ratio[block * rows : (block + 1) * rows]
        for c in range(tiles):
            at = slice(c * LANES, (c + 1) * LANES)
            out_ref[block, c * rows : (c + 1) * rows, :] = part[:, at]
            out_ref[block, tiles * rows + c : tiles * rows + c + 1, :] = running[:, at]
        running = jnp.maximum(running, jnp.max(jnp.abs(part), axis=0, keepdims=True))


def finish_kernel(upper_ref, message_ref, out_ref, peak_ref):
    _, length, _ = message_ref.shape
    rows, lanes = out_ref.shape
    tiles = (length - SUB) // rows
    blocks = lanes // (tiles * LANES)
    first = pl.program_id(0) * blocks
    upper = upper_ref[0] > 0
    row = lax.broadcasted_iota(jnp.int32, (rows, LANES), 0)
    for block in range(blocks):
        for c in range(tiles):
            start = (block * tiles + c) * LANES
            ratio = jnp.where(upper, message_ref[first + block, c * rows : (c + 1) * rows, :], 0.0)
            carry = jnp.where(upper, message_ref[first + block, tiles * rows + c : tiles * rows + c + 1, :], 0.0)
            peak = jnp.maximum(jnp.abs(ratio), carry)
            span = 1
            while span < rows:
                peak = jnp.maximum(peak, jnp.where(row >= span, pltpu.roll(peak, span, 0), 0.0))
                span *= 2
            out_ref[:, start : start + LANES] = ratio
            peak_ref[:, start : start + LANES] = peak


SMEM = pl.BlockSpec(memory_space=pltpu.SMEM)
GRANT = pltpu.CompilerParams(vmem_limit_bytes=12 << 20)
VMEM = pl.BlockSpec(memory_space=pltpu.VMEM)


def f32(*shape):
    return jax.ShapeDtypeStruct(shape, jnp.float32)


def per_device(values, cloud_words, history_len, monitor_start, boundary_table, devices):
    rows, pixels = values.shape
    dates = boundary_table.shape[0]
    half = devices // 2
    late = dates // 2
    width = pixels // half
    length = width // LANES * rows + SUB
    groups = [list(range(half)), list(range(half, devices))]
    upward = [(i, i + half) for i in range(half)]
    design = design_table(dates)
    spread = spread_table(width, max(1, rows // SUB))

    def exchange(blocks):
        return lax.all_to_all(blocks, AXES, 0, 0, axis_index_groups=groups, tiled=True)

    step_message = pl.BlockSpec((half // STEPS, length, LANES), lambda i: (i, 0, 0))
    step_pixels = pl.BlockSpec((rows, pixels // STEPS), lambda i: (0, i))
    step_words = pl.BlockSpec((rows, pixels // WORD // STEPS), lambda i: (0, i))
    message = pl.pallas_call(
        pack_kernel,
        grid=(STEPS,),
        out_shape=f32(half, length, LANES),
        in_specs=[step_pixels, step_words],
        out_specs=step_message,
        compiler_params=GRANT,
        name="pack",
    )(values, cloud_words)
    own = exchange(message)
    history = design[:late]
    base = (COLS + 1) * (width // LANES)
    stats, seen = pl.pallas_call(
        functools.partial(fit_kernel, rows=rows),
        out_shape=(f32(base + WINDOW // rows * length, LANES), f32(2 * late, width)),
        in_specs=[SMEM] + [VMEM] * 5,
        out_specs=(VMEM, VMEM),
        compiler_params=GRANT,
        name="fit",
    )(
        history_len,
        own,
        spread,
        np.concatenate(split_table(outer_table(history)), axis=0),
        np.concatenate(split_table(history.T), axis=0),
        six_wide(history),
    )
    piece = WINDOW // rows // STEPS * length

    def send(count):
        def branch(start, array, seen, bounds):
            stats = lax.ppermute(array[: base + count * piece], AXES, upward)
            return pl.pallas_call(
                functools.partial(ratio_kernel, rows=rows),
                out_shape=f32(half, length, LANES),
                in_specs=[SMEM] + [VMEM] * 5,
                out_specs=VMEM,
                compiler_params=GRANT,
                name="ratio",
            )(start, seen, stats, spread, six_wide(design[late - WINDOW :]), bounds)

        return branch

    reach = jnp.maximum(late + WINDOW - 1 - monitor_start[0], 0)
    message = lax.switch(
        (reach * STEPS + WINDOW - 1) // WINDOW,
        [send(count) for count in range(STEPS + 1)],
        monitor_start,
        stats,
        seen,
        boundary_table.reshape(1, dates),
    )
    upper = (lax.axis_index(AXES) >= half).astype(jnp.int32).reshape(1)
    return pl.pallas_call(
        finish_kernel,
        grid=(STEPS,),
        out_shape=(f32(rows, pixels), f32(rows, pixels)),
        in_specs=[SMEM, VMEM],
        out_specs=(step_pixels, step_pixels),
        compiler_params=GRANT,
        name="finish",
    )(upper, exchange(message))


def solution(mesh):
    placed = (P(AXES, None), P(AXES, None), P(), P(), P())
    return jax.shard_map(
        functools.partial(per_device, devices=mesh.size),
        mesh=mesh,
        in_specs=placed,
        out_specs=(P(AXES, None), P(AXES, None)),
        check_vma=False,
    )
```
